1024 devices in a mesh: grid: 32 (over z, x_hi), band: 32 (over y, x_lo, core).
Axes of the slice: x: 8 (x_hi: 4, x_lo: 2; x = x_hi * 2 + x_lo), y: 8, z: 8, core: 2. Of those that a mesh axis runs over, the one named last changes fastest.
Arguments:
- psi: bfloat16 [2048, 64, 512], P('band', 'grid'), may hold values from -6 to 6
- ritz_matrix: float32 [2048, 2048], P('band'), may hold values from -0.125 to 0.125
- potential: float32 [64, 512], P('grid'), may hold values from 0.5 to 10, as said below
Outputs:
- rotated: bfloat16 [2048, 64, 512], P('band', 'grid')
- search: bfloat16 [2048, 64, 512], P('band', 'grid')
The draws below stay inside these ranges and needn't reach their ends.
Inputs may be any that keep to these rules, and one draw needn't show every extreme that they name: `potential`: positive everywhere.
All inputs are finite; a program needn't handle non-finite values.
Results may differ from the reference program's by a relative error of at most 0.0049.
Values may be sent and summed in bfloat16 or wider, within the bound.
A program may use at most 32 MiB of HBM per device.

```python
import jax
import jax.numpy as jnp
from jax import lax

B = 2048
NY = 8
NZ = 64
NX = 64


def draw_potential(key, part):
    first_key = jax.random.fold_in(key, 11)
    rough = jnp.exp(jax.random.uniform(first_key, (NX, NY * NZ), jnp.float32, jnp.log(0.5), jnp.log(2.0)))
    ramp = 1.0 + 2.0 * jnp.arange(NX, dtype=jnp.float32)[:, None] / NX
    return rough * ramp


def steps_of(stream_key, shape, split, least, largest):
    loudness = 1.0
    for position, blocks in split:
        draws = jax.random.uniform(jax.random.fold_in(jax.random.fold_in(stream_key, 6), position), (blocks,), jnp.float32, least / len(split), largest / len(split))
        loudness = loudness * jnp.repeat(jnp.exp(draws), shape[position] // blocks).reshape((-1,) + (1,) * (len(shape) - 1 - position))
    return loudness


def gaussian(own_key, shape, spread, bound, cuts=(), kind=jnp.bfloat16):
    drawn = spread * jax.random.normal(own_key, shape, jnp.float32)
    if cuts:
        drawn = drawn * steps_of(own_key, shape, cuts, -0.22, 0.18)
    return jnp.clip(drawn, -bound, bound).astype(kind)


def setup_inputs(seed: int = 0) -> dict:
    splits = jax.random.split(jax.random.key(seed), 4)
    return {
        "psi": gaussian(splits[0], (B, NX, NY * NZ), 1.0, 6.0, ((0, 32), (1, 32))),
        "ritz_matrix": gaussian(splits[1], (B, B), B ** -0.5, 0.125, ((0, 32),), jnp.float32),
        "potential": draw_potential(jax.random.fold_in(splits[3], 71), 0),
    }


epsilon_mean = 1e-06

def reference(psi, ritz_matrix, potential):
    flattened = psi.reshape(B, -1).astype(jnp.float32)
    product = jnp.dot(ritz_matrix, flattened, precision=lax.Precision.HIGHEST)
    rotated = product.reshape(B, NX, NY * NZ).astype(jnp.bfloat16)
    center = rotated.astype(jnp.float32).reshape(B, NX, NY, NZ)
    laplacian = -6.0 * center
    for axis_number in (1, 2, 3):
        laplacian = laplacian + jnp.roll(center, 1, axis_number) + jnp.roll(center, -1, axis_number)
    field_pot = potential.reshape(1, NX, NY, NZ)
    resid = -0.5 * laplacian + field_pot * center
    total_cells = NX * NY * NZ
    m_cross = lax.optimization_barrier(jnp.sum(center * resid, axis=(1, 2, 3))) / total_cells
    m_self = lax.optimization_barrier(jnp.sum(center * center, axis=(1, 2, 3))) / total_cells + epsilon_mean
    ratio = m_cross / m_self
    direction = resid - ratio[:, None, None, None] * center
    m_dir = lax.optimization_barrier(jnp.sum(direction * direction, axis=(1, 2, 3))) / total_cells
    search = direction * lax.rsqrt(m_dir + epsilon_mean)[:, None, None, None]
    return (rotated, search.reshape(B, NX, NY * NZ).astype(jnp.bfloat16))
```

```python
import jax
import jax.numpy as jnp
from jax import lax
from jax.experimental import pallas as pl
from jax.experimental.pallas import tpu as pltpu
from jax.sharding import PartitionSpec as P

MESH = pl.DeviceIdType.MESH
F32 = jnp.float32
BF16 = jnp.bfloat16

ZS = 8
XHS = 4
YS = 8
GRID = ZS * XHS
ROWS = 64
CELLS = 512
HALF = CELLS // 2
QUAD = 4 * ROWS
BANDS = YS * QUAD
EPS = 1e-06
TOTAL = 64 * CELLS
LANES = 128


def kernel(
    psi_ref, ritz_ref, pot_ref, rot_ref, search_ref,
    gath, lhs, acc, rv, planes, other, resid, st1, st2,
    ritz_sem, ring_send, ring_recv, sib_send, sib_recv, x_send, x_recv,
    r_send, r_recv, halo_send, halo_recv, s1_send, s1_recv, s2_send, s2_recv,
):
    g = lax.axis_index("grid")
    b = lax.axis_index("band")
    z, xh = lax.div(g, XHS), lax.rem(g, XHS)
    y, xl, c = lax.div(b, 4), lax.rem(lax.div(b, 2), 2), lax.rem(b, 2)

    def band_of(y_, xl_, c_):
        return (y_ * 2 + xl_) * 2 + c_

    def grid_of(z_, xh_):
        return z_ * XHS + xh_

    up = (g, band_of(lax.rem(y + 1, YS), xl, c))
    down = (g, band_of(lax.rem(y + YS - 1, YS), xl, c))
    sib = (g, band_of(y, xl, 1 - c))
    partner = (g, band_of(y, 1 - xl, c))
    outer = (grid_of(z, lax.rem(xh + 2 * xl - 1 + XHS, XHS)), band_of(y, 1 - xl, c))
    g_to = lax.rem(g + 2 * xl - 1 + GRID, GRID)
    g_from = lax.rem(g + 1 - 2 * xl + GRID, GRID)
    halo_own = (g_to, b)
    halo_back = (g_from, b)
    halo_cross = (g_to, band_of(y, 1 - xl, c))
    x_peers = [(grid_of(z, lax.rem(xh + i, XHS)), b) for i in range(1, XHS)]
    z_peers = [(grid_of(lax.rem(z + i, ZS), xh), b) for i in range(1, ZS)]

    ritz_copy = pltpu.make_async_copy(ritz_ref, rv.at[xl], ritz_sem)
    ritz_copy.start()

    barrier = pltpu.get_barrier_semaphore()
    greeted = [up, down, sib, partner, outer, halo_own, halo_back, halo_cross] + x_peers + z_peers
    for device in greeted:
        pl.semaphore_signal(barrier, inc=1, device_id=device, device_id_type=MESH)
    pl.semaphore_wait(barrier, len(greeted))

    sent = []

    def copy_of(src, dst, send_sem, recv_sem, device):
        return pltpu.make_async_remote_copy(
            src_ref=src, dst_ref=dst, send_sem=send_sem, recv_sem=recv_sem,
            device_id=device, device_id_type=MESH,
        )

    def send(*args):
        copy = copy_of(*args)
        copy.start()
        sent.append(copy)

    def arrived(ref, send_sem, recv_sem):
        copy_of(ref, ref, send_sem, recv_sem, sib).wait_recv()

    row = [pl.multiple_of((xl * 2 + c) * ROWS, ROWS), pl.multiple_of(((1 - xl) * 2 + c) * ROWS, ROWS)]
    sib_row = [
        pl.multiple_of((xl * 2 + 1 - c) * ROWS, ROWS),
        pl.multiple_of(((1 - xl) * 2 + 1 - c) * ROWS, ROWS),
    ]

    def cells(q):
        return pl.ds(q * HALF, HALF)

    def chunk(rel, kind, q):
        return gath.at[rel, pl.ds(row[kind], ROWS), cells(q)]

    def sib_chunk(rel, kind, q):
        return gath.at[rel, pl.ds(sib_row[kind], ROWS), cells(q)]

    def to_up(src, rel, kind, q):
        send(src, chunk(rel + 1, kind, q), ring_send.at[0, rel, kind, q], ring_recv.at[rel + 1, kind, q], up)

    def to_down(src, rel, kind, q):
        to = (rel + YS - 1) % YS
        send(src, chunk(to, kind, q), ring_send.at[1, (YS - rel) % YS, kind, q], ring_recv.at[to, kind, q], down)

    def to_sib(src, rel, kind, q):
        send(src, chunk(rel, kind, q), sib_send.at[rel, kind, q], sib_recv.at[rel, kind, q], sib)

    def ring_arrived(rel, kind, q):
        arrived(chunk(rel, kind, q), sib_send.at[rel, kind, q], ring_recv.at[rel, kind, q])

    def sib_arrived(rel, kind, q):
        arrived(sib_chunk(rel, kind, q), sib_send.at[rel, kind, q], sib_recv.at[rel, kind, q])

    for q in range(2):
        send(psi_ref.at[1 - xl, :, cells(q)], chunk(0, 0, q), x_send.at[q], x_recv.at[q], partner)
    for q in range(2):
        src = psi_ref.at[xl, :, cells(q)]
        to_up(src, 0, 0, q)
        to_down(src, 0, 0, q)
        to_sib(src, 0, 0, q)

    ritz_copy.wait()
    part = ROWS // 2
    send(rv.at[xl, pl.ds(0, part)], rv.at[xl, pl.ds(0, part)], r_send.at[0], r_recv.at[0], partner)
    send(rv.at[xl, pl.ds(part, part)], rv.at[xl, pl.ds(part, part)], r_send.at[1], r_recv.at[1], outer)

    gath[0, pl.ds(row[0], ROWS), :] = psi_ref[xl]

    def split_ritz(who):
        hi_at = pl.ds(pl.multiple_of(who * ROWS, ROWS), ROWS)
        lo_at = pl.ds(pl.multiple_of(2 * ROWS + who * ROWS, ROWS), ROWS)
        for yy in range(YS):
            value = rv[who, :, yy * QUAD : (yy + 1) * QUAD]
            high = value.astype(BF16)
            lhs[yy, hi_at, :] = high
            lhs[yy, lo_at, :] = (value - high.astype(F32)).astype(BF16)

    split_ritz(xl)

    for q in range(2):
        arrived(chunk(0, 1, q), x_send.at[q], x_recv.at[q])
        src = chunk(0, 1, q)
        to_up(src, 0, 1, q)
        to_down(src, 0, 1, q)
        to_sib(src, 0, 1, q)

    first = [True, True]

    def multiply(rel, q):
        for kind in range(2):
            sib_arrived(rel, kind, q)
        owner = lax.rem(y - rel + YS, YS)
        term = jnp.dot(lhs[owner], gath[rel, :, q * HALF : (q + 1) * HALF], preferred_element_type=F32)
        if first[q]:
            acc[q] = term
            first[q] = False
        else:
            acc[q] += term

    def handle(d, kind, q):
        rel = d
        ring_arrived(rel, kind, q)
        if d < 3 or kind == 0:
            to_up(chunk(rel, kind, q), rel, kind, q)
        to_sib(chunk(rel, kind, q), rel, kind, q)
        rel = YS - d
        ring_arrived(rel, kind, q)
        if d < 3 or kind == 1:
            to_down(chunk(rel, kind, q), rel, kind, q)
        to_sib(chunk(rel, kind, q), rel, kind, q)

    for d in (1, 2):
        for kind in range(2):
            for q in range(2):
                handle(d, kind, q)

    handle(3, 0, 0)
    arrived(rv.at[1 - xl, pl.ds(0, part)], r_send.at[0], r_recv.at[0])
    arrived(rv.at[1 - xl, pl.ds(part, part)], r_send.at[1], r_recv.at[1])
    split_ritz(1 - xl)
    handle(3, 0, 1)
    for rel in (0, 1):
        for q in range(2):
            multiply(rel, q)
    handle(3, 1, 0)
    for rel in (7, 2):
        for q in range(2):
            multiply(rel, q)
    handle(3, 1, 1)
    for q in range(2):
        multiply(6, q)
    for rel in (3, 5):
        for q in range(2):
            multiply(rel, q)

    slot = 3 * (1 - xl)
    for q in range(2):
        at = slice(q * HALF, (q + 1) * HALF)
        for kind in range(2):
            ring_arrived(4, kind, q)
            to_sib(chunk(4, kind, q), 4, kind, q)
        multiply(4, q)

        def rows_of(who):
            high = acc[q, pl.ds(pl.multiple_of(who * ROWS, ROWS), ROWS), :]
            low = acc[q, pl.ds(pl.multiple_of(2 * ROWS + who * ROWS, ROWS), ROWS), :]
            return (high + low).astype(BF16)

        other[:, at] = rows_of(1 - xl)
        planes[1 + xl, :, at] = rows_of(xl)
        src = other.at[:, cells(q)]
        send(src, planes.at[1 + xl, :, cells(q)], halo_send.at[0, q], halo_recv.at[1 + xl, q], partner)
        send(src, planes.at[slot, :, cells(q)], halo_send.at[1, q], halo_recv.at[slot, q], halo_cross)
        src = planes.at[1 + xl, :, cells(q)]
        send(src, planes.at[slot, :, cells(q)], halo_send.at[2, q], halo_recv.at[slot, q], halo_own)

    for q in range(2):
        for at in (0, 2 - xl, 3):
            arrived(planes.at[at, :, cells(q)], halo_send.at[0, q], halo_recv.at[at, q])

    lane = lax.broadcasted_iota(jnp.int32, (ROWS, LANES), 1)
    low_half = lane < 64
    z_last = lax.rem(lane, 64) == 63
    z_first = lax.rem(lane, 64) == 0
    tiles = CELLS // LANES
    sums = [None, None, None]
    for p in range(2):
        center = [planes[1 + p, :, t * LANES : (t + 1) * LANES].astype(F32) for t in range(tiles)]
        turned = [pltpu.roll(v, 64, 1) for v in center]
        for t in range(tiles):
            at = slice(t * LANES, (t + 1) * LANES)
            v = center[t]
            below = planes[p, :, at].astype(F32)
            above = planes[p + 2, :, at].astype(F32)
            across_y = turned[t] + jnp.where(low_half, turned[(t + tiles - 1) % tiles], turned[(t + 1) % tiles])
            after = jnp.where(z_last, pltpu.roll(v, 63, 1), pltpu.roll(v, LANES - 1, 1))
            before = jnp.where(z_first, pltpu.roll(v, LANES - 63, 1), pltpu.roll(v, 1, 1))
            laplacian = (below + above) + across_y + (after + before) - 6.0 * v
            value = -0.5 * laplacian + pot_ref[p : p + 1, at] * v
            resid[p, :, at] = value
            for i, term in enumerate((v * value, v * v, value * value)):
                sums[i] = term if sums[i] is None else sums[i] + term
        rot_ref[p] = planes[1 + p]

    cols = [jnp.sum(s, axis=1, keepdims=True) for s in sums]
    packed = jnp.where(lane == 0, cols[0], jnp.where(lane == 1, cols[1], jnp.where(lane == 2, cols[2], 0.0)))
    square = jnp.concatenate([packed, jnp.zeros((LANES - ROWS, LANES), F32)], axis=0)
    st1[0] = jnp.transpose(square)[0:8]
    for i, device in enumerate(x_peers, 1):
        send(st1.at[0], st1.at[i], s1_send.at[i], s1_recv.at[i], device)
    for i in range(1, XHS):
        arrived(st1.at[i], s1_send.at[i], s1_recv.at[i])
    st2[0] = (st1[0] + st1[1]) + (st1[2] + st1[3])
    for i, device in enumerate(z_peers, 1):
        send(st2.at[0], st2.at[i], s2_send.at[i], s2_recv.at[i], device)
    total = st2[0]
    for i in range(1, ZS):
        arrived(st2.at[i], s2_send.at[i], s2_recv.at[i])
        total = total + st2[i]
    total = total / TOTAL
    m_cross, m_plain, m_resid = total[0:1], total[1:2], total[2:3]
    ratio = m_cross / (m_plain + EPS)
    m_dir = m_resid - 2.0 * ratio * m_cross + ratio * ratio * m_plain
    scale = lax.rsqrt(m_dir + EPS)
    line = lax.broadcasted_iota(jnp.int32, (LANES, LANES), 0)
    both = jnp.transpose(jnp.where(line == 0, ratio, jnp.where(line == 1, scale, 0.0)))
    ratio_col, scale_col = both[0:ROWS, 0:1], both[0:ROWS, 1:2]
    for p in range(2):
        for t in range(tiles):
            at = slice(t * LANES, (t + 1) * LANES)
            v = planes[1 + p, :, at].astype(F32)
            search_ref[p, :, at] = ((resid[p, :, at] - ratio_col * v) * scale_col).astype(BF16)

    for copy in sent:
        copy.wait_send()


def shards(psi, ritz_matrix, potential):
    dma = pltpu.SemaphoreType.DMA
    vmem = pl.BlockSpec(memory_space=pltpu.VMEM)
    shape = jax.ShapeDtypeStruct((2, ROWS, CELLS), BF16)
    rotated, search = pl.pallas_call(
        kernel,
        out_shape=(shape, shape),
        in_specs=[vmem, pl.BlockSpec(memory_space=pltpu.HBM), vmem],
        out_specs=(vmem, vmem),
        scratch_shapes=[
            pltpu.VMEM((YS, QUAD, CELLS), BF16),
            pltpu.VMEM((YS, QUAD, QUAD), BF16),
            pltpu.VMEM((2, QUAD, HALF), F32),
            pltpu.VMEM((2, ROWS, BANDS), F32),
            pltpu.VMEM((4, ROWS, CELLS), BF16),
            pltpu.VMEM((ROWS, CELLS), BF16),
            pltpu.VMEM((2, ROWS, CELLS), F32),
            pltpu.VMEM((XHS, 8, LANES), F32),
            pltpu.VMEM((ZS, 8, LANES), F32),
            dma(()),
            dma((2, 4, 2, 2)),
            dma((YS, 2, 2)),
            dma((YS, 2, 2)),
            dma((YS, 2, 2)),
            dma((2,)),
            dma((2,)),
            dma((2,)),
            dma((2,)),
            dma((3, 2)),
            dma((4, 2)),
            dma((XHS,)),
            dma((XHS,)),
            dma((ZS,)),
            dma((ZS,)),
        ],
        compiler_params=pltpu.CompilerParams(
            collective_id=0, has_side_effects=True, vmem_limit_bytes=32 * 1024 * 1024
        ),
    )(jnp.transpose(psi, (1, 0, 2)), ritz_matrix, potential)
    return (jnp.transpose(rotated, (1, 0, 2)), jnp.transpose(search, (1, 0, 2)))


def solution(mesh):
    return jax.shard_map(
        shards,
        mesh=mesh,
        in_specs=(P("band", "grid", None), P("band", None), P("grid", None)),
        out_specs=(P("band", "grid", None), P("band", "grid", None)),
        check_vma=False,
    )
```
